512 devices in a mesh: clip: 4 (over y_lo, core), seq: 128 (over y_hi, z, x).
Axes of the slice: x: 4, y: 4 (y_hi: 2, y_lo: 2; y = y_hi * 2 + y_lo), z: 16, core: 2. Of those that a mesh axis runs over, the one named last changes fastest.
Arguments:
- temporal_queries: bfloat16 [512, 128, 1152], P(('clip', 'seq')), parts along dimension 0, may hold values from -6 to 6
- temporal_keys: bfloat16 [512, 128, 1152], P(('clip', 'seq')), parts along dimension 0, may hold values from -6 to 6
- temporal_values: bfloat16 [512, 128, 1152], P(('clip', 'seq')), parts along dimension 0, may hold values from -6 to 6
- temporal_cotangent: bfloat16 [512, 128, 1152], P(('clip', 'seq')), parts along dimension 0, may hold values from -6 to 6
- cross_queries: bfloat16 [512, 128, 1152], P(('clip', 'seq')), parts along dimension 0, may hold values from -6 to 6
- cross_cotangent: bfloat16 [512, 128, 1152], P(('clip', 'seq')), parts along dimension 0, may hold values from -24 to 24
- text_keys: bfloat16 [640, 1152], P('clip'), parts along dimension 0, may hold values from -6 to 6
- text_values: bfloat16 [640, 1152], P('clip'), parts along dimension 0, may hold values from -6 to 6
- text_length: int32 [4], P('clip'), parts along dimension 0, may hold values from 80 to 160
Outputs:
- temporal_queries_grad: bfloat16 [512, 128, 1152], P(('clip', 'seq')), parts along dimension 0
- temporal_keys_grad: bfloat16 [512, 128, 1152], P(('clip', 'seq')), parts along dimension 0
- temporal_values_grad: bfloat16 [512, 128, 1152], P(('clip', 'seq')), parts along dimension 0
- cross_queries_grad: bfloat16 [512, 128, 1152], P(('clip', 'seq')), parts along dimension 0
- text_kv_grad: float32 [640, 2304], P('clip', 'seq'), parts along dimension 0
The draws below stay inside these ranges and needn't reach their ends.
There are 4 independent parts, one for each index of `clip`. The reference program is written for one: setup_inputs(seed, part) draws one part's arguments, and reference() takes and returns one part's arrays. A program takes and returns all parts, laid end to end along the dimension named above; each array names one. Nothing has to cross between parts.
All inputs are finite; a program needn't handle non-finite values.
Results may differ from the reference program's by a relative error of at most 0.012.
The reference program's roundings to bfloat16 on the way count: a program that leaves them out, or rounds other values in their place, can miss the bound.
Values may be sent and summed in bfloat16 or wider, within the bound.
A program may use at most 64 MiB of HBM per device.

```python
import math
import jax
import jax.numpy as jnp
from jax import lax

D = 1152
HEADS = 16
TEXT = 160
HEAD_DIM = 72
POS = 128
FRAMES = 128


def base_field(key, extent):
    return jnp.clip(jax.random.normal(key, extent, jnp.float32), -6.0, 6.0)


def temporal_pair(key):
    key_query, key_target = jax.random.split(jax.random.fold_in(key, 101), 2)
    queries = base_field(key_query, (FRAMES, POS, D))
    targets = base_field(key_target, (FRAMES, POS, D))
    return (queries, targets)


def cross_pair(key):
    key_query, key_target = jax.random.split(jax.random.fold_in(key, 202), 2)
    queries = base_field(key_query, (FRAMES, POS, D))
    targets = base_field(key_target, (TEXT, D))
    return (queries, targets)


def draw_temporal_queries(key, part):
    return temporal_pair(key)[0].astype(jnp.bfloat16)


def draw_temporal_keys(key, part):
    return temporal_pair(key)[1].astype(jnp.bfloat16)


def draw_cross_queries(key, part):
    return cross_pair(key)[0].astype(jnp.bfloat16)


def draw_text_keys(key, part):
    return cross_pair(key)[1].astype(jnp.bfloat16)


def raised(values, rng, source, target, shards_of, factor):
    owner, partner = [(jnp.arange(values.shape[axis_at]) // (values.shape[axis_at] // shards_of)).reshape([-1 if axis == axis_at else 1 for axis in range(values.ndim)]) for axis_at in (source, target)]
    chosen = jax.random.permutation(rng, shards_of)[partner]
    strong = (owner == chosen) | (owner == (partner + shards_of // 2) % shards_of)
    return jnp.where(strong, factor * values, values)


def steps_of(own_key, dims, cuts, least, top_value):
    def one(dim, blocks):
        steps = jax.random.uniform(jax.random.fold_in(jax.random.fold_in(own_key, 6), dim), (blocks,), jnp.float32, least / len(cuts), top_value / len(cuts))
        return jnp.repeat(jnp.exp(steps), dims[dim] // blocks).reshape((-1,) + (1,) * (len(dims) - dim - 1))

    loudness = one(*cuts[0])
    for cut in cuts[1:]:
        loudness = loudness * one(*cut)
    return loudness


def scatter_about(rng, shape, deviation, bound, shards=(), kind=jnp.bfloat16):
    entries = jax.random.normal(rng, shape, jnp.float32) * deviation
    if len(shards) > 0:
        entries = steps_of(rng, shape, shards, -0.22, 0.18) * entries
    return jnp.clip(entries, min=-bound, max=bound).astype(kind)


def gaussian_with(key, shape, scale, reach, cuts, heavy, kind=jnp.bfloat16):
    values = scale * jax.random.normal(key, shape, jnp.float32)
    if cuts:
        values = values * steps_of(key, shape, cuts, -0.22, 0.18)
    return jnp.clip(raised(values, jax.random.fold_in(key, 3), *heavy), -reach, reach).astype(kind)


def setup_inputs(seed: int = 0, part: int = 0) -> dict:
    splits = jax.random.split(jax.random.key(seed), 10)
    part_keys = jax.random.split(jax.random.fold_in(splits[9], part), 10)
    temporal_queries = draw_temporal_queries(jax.random.fold_in(jax.random.fold_in(splits[9], part), 71), part)
    temporal_keys = draw_temporal_keys(jax.random.fold_in(jax.random.fold_in(splits[9], part), 71), part)
    temporal_values = scatter_about(part_keys[2], (FRAMES, POS, D), 1.0, 6.0, ((0, 128),))
    temporal_cotangent = scatter_about(part_keys[3], (FRAMES, POS, D), 1.0, 6.0, ((0, 128),))
    cross_queries = draw_cross_queries(jax.random.fold_in(jax.random.fold_in(splits[9], part), 71), part)
    cross_cotangent = gaussian_with(part_keys[5], (FRAMES, POS, D), 1.0, 24.0, ((0, 128),), (0, 2, 128, 5.5))
    text_keys = draw_text_keys(jax.random.fold_in(jax.random.fold_in(splits[9], part), 71), part)
    text_values = scatter_about(part_keys[7], (TEXT, D), 1.0, 6.0)
    text_length = jax.random.randint(part_keys[8], (1,), TEXT // 2, TEXT + 1).astype(jnp.int32)
    return {"temporal_queries": temporal_queries, "temporal_keys": temporal_keys, "temporal_values": temporal_values, "temporal_cotangent": temporal_cotangent, "cross_queries": cross_queries, "cross_cotangent": cross_cotangent, "text_keys": text_keys, "text_values": text_values, "text_length": text_length}


def attend_back(queries, targets, values, cotangent, keep, scale):
    highest = lax.Precision.HIGHEST
    query_f = queries.astype(jnp.float32)
    target_f = targets.astype(jnp.float32)
    value_f = values.astype(jnp.float32)
    cotan_f = cotangent.astype(jnp.float32)
    scores = jnp.einsum('mhe,nhe->hmn', query_f, target_f, precision=highest) * scale
    if keep is not None:
        scores = jnp.where(keep, scores, -1e+30)
    highest_score = lax.optimization_barrier(jnp.max(scores, axis=-1, keepdims=True))
    expo = jnp.exp(scores - highest_score)
    weights = expo / lax.optimization_barrier(jnp.sum(expo, axis=-1, keepdims=True))
    rounded = lax.optimization_barrier(weights.astype(jnp.bfloat16)).astype(jnp.float32)
    output = jnp.einsum('hmn,nhe->mhe', rounded, value_f, precision=highest)
    deltas = lax.optimization_barrier(jnp.sum(cotan_f * output, axis=-1))
    grad_values = jnp.einsum('hmn,mhe->nhe', rounded, cotan_f, precision=highest)
    products = jnp.einsum('mhe,nhe->hmn', cotan_f, value_f, precision=highest)
    slopes = weights * (products - jnp.transpose(deltas)[:, :, None]) * scale
    sloped = lax.optimization_barrier(slopes.astype(jnp.bfloat16)).astype(jnp.float32)
    grad_queries = jnp.einsum('hmn,nhe->mhe', sloped, target_f, precision=highest)
    grad_targets = jnp.einsum('hmn,mhe->nhe', sloped, query_f, precision=highest)
    return (grad_queries, grad_targets, grad_values)

def reference(temporal_queries, temporal_keys, temporal_values, temporal_cotangent, cross_queries, cross_cotangent, text_keys, text_values, text_length):
    scale = 1.0 / math.sqrt(HEAD_DIM)

    def split_heads(array):
        return array.reshape(FRAMES, POS, HEADS, HEAD_DIM).transpose(1, 0, 2, 3)

    def merge_heads(array):
        return array.transpose(1, 0, 2, 3).reshape(FRAMES, POS, D).astype(jnp.bfloat16)

    def one_column(group):
        return attend_back(group[0], group[1], group[2], group[3], None, scale)
    grad_query, grad_key, grad_value = lax.map(one_column, (split_heads(temporal_queries), split_heads(temporal_keys), split_heads(temporal_values), split_heads(temporal_cotangent)))
    keep = (jnp.arange(TEXT, dtype=jnp.int32) < text_length[0].astype(jnp.int32))[None, None, :]
    text_heads = text_keys.reshape(TEXT, HEADS, HEAD_DIM)
    value_heads = text_values.reshape(TEXT, HEADS, HEAD_DIM)

    def one_frame(carry, group):
        frame_query = group[0].reshape(POS, HEADS, HEAD_DIM)
        frame_cotan = group[1].reshape(POS, HEADS, HEAD_DIM)
        grads = attend_back(frame_query, text_heads, value_heads, frame_cotan, keep, scale)
        return ((carry[0] + grads[1], carry[1] + grads[2]), grads[0].reshape(POS, D).astype(jnp.bfloat16))
    zeros = jnp.zeros((TEXT, HEADS, HEAD_DIM), jnp.float32)
    sums, cross_grad = lax.scan(one_frame, (zeros, zeros), (cross_queries, cross_cotangent))
    text_grad = jnp.concatenate([sums[0], sums[1]], axis=2).reshape(TEXT, 2 * D)
    return (merge_heads(grad_query), merge_heads(grad_key), merge_heads(grad_value), cross_grad, text_grad)
```

```python
import math

import jax
import jax.numpy as jnp
from jax import lax
from jax.experimental import pallas as pl
from jax.experimental.pallas import tpu as pltpu
from jax.sharding import Mesh
from jax.sharding import PartitionSpec as P

HEADS = 16
HEAD_DIM = 72
WIDTH = HEADS * HEAD_DIM
POS = 128
TEXT = 160
NZ = 16
NX = 4
NPL = 8
SCALE = 1.0 / math.sqrt(HEAD_DIM)
CLIP_SEQ = ("clip", "seq_0", "seq_1", "seq_2")
SEQ = ("seq_0", "seq_1", "seq_2")
MESH = pl.DeviceIdType.MESH
BF = jnp.bfloat16
F32 = jnp.float32

IN_CHUNKS = ((0, 640), (640, 512))
HEAD_CHUNKS = ((0, 8), (8, 16))
OUT_CHUNKS = ((0, 512), (512, 640))
DISTANCES = (8, 7, 9, 6, 10, 5, 11, 4, 12, 3, 13, 2, 14, 1, 15)
TEXT_ROWS = TEXT // NX
HALF = 640


def window(head):
    low = HEAD_DIM * head // 128 * 128
    return low, -(-HEAD_DIM * (head + 1) // 128) * 128


def head_mask(head):
    low, high = window(head)
    lane = lax.broadcasted_iota(jnp.int32, (1, high - low), 1) + low
    inside = (lane >= HEAD_DIM * head) & (lane < HEAD_DIM * (head + 1))
    return jnp.where(inside, 1.0, 0.0).astype(BF)


def across(a, b):
    return lax.dot_general(a, b, (((1,), (1,)), ((), ())), preferred_element_type=F32)


def down(a, b):
    return lax.dot_general(a, b, (((0,), (0,)), ((), ())), preferred_element_type=F32)


def head_back(q, k, v, g, mask, keep):
    kz, vz, qz, gz = k * mask, v * mask, q * mask, g * mask
    scores = across(kz, q) * SCALE
    if keep is not None:
        scores = jnp.where(keep, scores, -1e30)
    expo = jnp.exp(scores - jnp.max(scores, axis=0, keepdims=True))
    weights = expo * (1.0 / jnp.sum(expo, axis=0, keepdims=True))
    rounded = weights.astype(BF)
    products = across(vz, g)
    delta = jnp.sum(rounded.astype(F32) * products, axis=0, keepdims=True)
    slopes = (weights * (products - delta) * SCALE).astype(BF)
    grad_v = jnp.dot(rounded, gz, preferred_element_type=F32)
    grad_k = jnp.dot(slopes, qz, preferred_element_type=F32)
    grad_q = down(slopes, kz)
    return grad_q, grad_k, grad_v


class Tiles:
    def __init__(self, store):
        self.open, self.store = {}, store

    def add(self, head, value):
        low, high = window(head)
        for t in range(low // 128, high // 128):
            part = value[:, 128 * t - low : 128 * t - low + 128]
            self.open[t] = part if t not in self.open else self.open[t] + part
            if HEAD_DIM * (head + 1) >= 128 * (t + 1):
                self.store(t, self.open.pop(t))


def kernel(
    tq, tk, tv, tg, cq, cg, xk, xv, length,
    oq, ok, ov, ocq, otext,
    zbuf, pout, pbuf, gbuf, qbuf, zout, tall, tpart, rs1, rs2out, rs2, rs3out, rs3,
    zs, zr, ps, pr, qs, qr, ws, wr, ts, tr,
):
    y, z, x = lax.axis_index("seq_0"), lax.axis_index("seq_1"), lax.axis_index("seq_2")
    me = y * NX + x
    ins, outs = (tq, tk, tv, tg), (oq, ok, ov)

    def z_peer(k):
        return lax.rem(z + k, NZ)

    def plane_peer(k):
        return lax.rem(y + k // NX, 2), lax.rem(x + k % NX, NX)

    def in_plane(k):
        py, px = plane_peer(k)
        return {"seq_0": py, "seq_2": px}

    barrier = pltpu.get_barrier_semaphore()
    for k in range(1, NZ):
        pl.semaphore_signal(barrier, 1, device_id={"seq_1": z_peer(k)}, device_id_type=MESH)
    for k in range(1, NPL):
        pl.semaphore_signal(barrier, 1, device_id=in_plane(k), device_id_type=MESH)
    pl.semaphore_wait(barrier, NZ - 1 + NPL - 1)

    def send(src, dst, send_sem, recv_sem, device):
        pltpu.make_async_remote_copy(
            src_ref=src, dst_ref=dst, send_sem=send_sem, recv_sem=recv_sem, device_id=device, device_id_type=MESH
        ).start()

    def wait_for(ref, sem):
        pltpu.make_async_copy(ref, ref, sem).wait()

    for c, (low, size) in enumerate(IN_CHUNKS):
        lanes = pl.ds(low, size)
        for a in range(4):
            for k in DISTANCES:
                peer = z_peer(k)
                send(ins[a].at[peer, :, lanes], zbuf.at[a, z, :, lanes], zs.at[c, a], zr.at[c, a], {"seq_1": peer})
    for a in range(4):
        zbuf[a, z] = ins[a][z]

    text_rows = lax.broadcasted_iota(jnp.int32, (TEXT, POS), 0)
    keep = text_rows < length[0]

    def put_cross(t, value):
        ocq[:, 128 * t : 128 * t + 128] = value.astype(BF)

    def put_text(kind):
        def put(t, value):
            tpart[kind, :, 128 * t : 128 * t + 128] = value

        return put

    sums = (Tiles(put_cross), Tiles(put_text(0)), Tiles(put_text(1)))
    for h in range(HEADS):
        low, high = window(h)
        grads = head_back(cq[:, low:high], xk[:, low:high], xv[:, low:high], cg[:, low:high], head_mask(h), keep)
        for s, grad in zip(sums, grads, strict=True):
            s.add(h, grad)

    for k in range(1, NPL):
        py, px = plane_peer(k)
        rows, lanes = pl.ds(pl.multiple_of(px * TEXT_ROWS, 8), TEXT_ROWS), pl.ds(pl.multiple_of(py * 512, 128), HALF)
        send(tpart.at[:, rows, lanes], rs1.at[me], ts.at[0], tr.at[0], in_plane(k))
    own_rows, own_lanes = pl.ds(pl.multiple_of(x * TEXT_ROWS, 8), TEXT_ROWS), pl.ds(pl.multiple_of(y * 512, 128), HALF)
    rs1[me] = tpart[:, own_rows, own_lanes]

    def hand_on(c):
        low, size = IN_CHUNKS[c]
        lanes = pl.ds(low, size)
        for a in range(4):
            wait_for(zbuf.at[a, pl.ds(0, NZ - 1), :, lanes], zr.at[c, a])
            for t in range(low, low + size, 128):
                for f in range(NZ):
                    tall[t // 128, pl.ds(f, NPL, stride=NZ), :] = zbuf[a, f, :, t : t + 128].astype(F32)
                for j in range(NPL):
                    pout[a, j, :, t : t + 128] = tall[t // 128, NZ * j : NZ * j + NZ, :].astype(BF)
            for k in range(1, NPL):
                py, px = plane_peer(k)
                send(pout.at[a, py * NX + px, :, lanes], pbuf.at[a, me, :, lanes], ps.at[c, a], pr.at[c, a], in_plane(k))
            pbuf[a, me, :, low : low + size] = pout[a, me, :, low : low + size]

    def put_temporal(a):
        def put(t, value):
            gbuf[a, :, :, 128 * t : 128 * t + 128] = value.astype(BF).reshape(NPL, NZ, 128)

        return put

    temporal = tuple(Tiles(put_temporal(a)) for a in range(3))

    def attend(c):
        low, size = IN_CHUNKS[c]
        for a in range(4):
            wait_for(pbuf.at[a, pl.ds(0, NPL - 1), :, pl.ds(low, size)], pr.at[c, a])
        for h in range(*HEAD_CHUNKS[c]):
            lo, hi = window(h)
            q, k, v, g = (pbuf[a, :, :, lo:hi].reshape(POS, hi - lo) for a in range(4))
            for s, grad in zip(temporal, head_back(q, k, v, g, head_mask(h), None), strict=True):
                s.add(h, grad)

    def give_back(c):
        low, size = OUT_CHUNKS[c]
        lanes = pl.ds(low, size)
        for a in range(3):
            for k in range(1, NPL):
                py, px = plane_peer(k)
                send(gbuf.at[a, py * NX + px, :, lanes], qbuf.at[a, me, :, lanes], qs.at[c, a], qr.at[c, a], in_plane(k))
            qbuf[a, me, :, low : low + size] = gbuf[a, me, :, low : low + size]

    def deliver(c):
        low, size = OUT_CHUNKS[c]
        lanes = pl.ds(low, size)
        for a in range(3):
            wait_for(qbuf.at[a, pl.ds(0, NPL - 1), :, lanes], qr.at[c, a])
            for t in range(low, low + size, 128):
                for j in range(NPL):
                    tall[t // 128, pl.ds(j, NZ, stride=NPL), :] = qbuf[a, j, :, t : t + 128].astype(F32)
                for f in range(NZ):
                    zout[a, f, :, t : t + 128] = tall[t // 128, NPL * f : NPL * f + NPL, :].astype(BF)
            for k in DISTANCES:
                peer = z_peer(k)
                send(zout.at[a, peer, :, lanes], outs[a].at[z, :, lanes], ws.at[c, a], wr.at[c, a], {"seq_1": peer})
            outs[a][z, :, low : low + size] = zout[a, z, :, low : low + size]

    hand_on(0)

    wait_for(rs1.at[pl.ds(0, NPL - 1)], tr.at[0])
    for kind in range(2):
        total = rs1[0, kind]
        for j in range(1, NPL):
            total = total + rs1[j, kind]
        for i in range(HEADS // 2):
            first, second = (total[:, s : s + HEAD_DIM] for s in (HEAD_DIM * i, HEAD_DIM * i + 64))
            block = jnp.where(y == 0, first, second)
            rs2out[2 * i + kind] = jnp.pad(block, ((0, 0), (0, 128 - HEAD_DIM))).astype(BF)
    for k in DISTANCES:
        peer = z_peer(k)
        send(rs2out.at[peer], rs2.at[z], ts.at[1], tr.at[1], {"seq_1": peer})
    rs2[z] = rs2out[z]

    attend(0)
    give_back(0)
    hand_on(1)
    deliver(0)

    wait_for(rs2.at[pl.ds(0, NZ - 1)], tr.at[1])
    total = rs2[0].astype(F32)
    for f in range(1, NZ):
        total = total + rs2[f].astype(F32)
    columns = HEAD_DIM // NX
    for j in range(NX):
        rs3out[j] = jnp.pad(total[:, columns * j : columns * j + columns], ((0, 0), (0, 128 - columns)))
    for k in range(1, NX):
        _, px = plane_peer(k)
        send(rs3out.at[px], rs3.at[x], ts.at[2], tr.at[2], in_plane(k))
    rs3[x] = rs3out[x]

    attend(1)
    give_back(1)
    deliver(1)

    wait_for(rs3.at[pl.ds(0, NX - 1)], tr.at[2])
    for j in range(NX):
        otext[TEXT_ROWS * j : TEXT_ROWS * j + TEXT_ROWS, :] = rs3[j]

    for c in range(2):
        lanes_in, lanes_out = pl.ds(*IN_CHUNKS[c]), pl.ds(*OUT_CHUNKS[c])
        for a in range(4):
            wait_for(zbuf.at[a, pl.ds(0, NZ - 1), :, lanes_in], zs.at[c, a])
            wait_for(pout.at[a, pl.ds(0, NPL - 1), :, lanes_in], ps.at[c, a])
        for a in range(3):
            wait_for(gbuf.at[a, pl.ds(0, NPL - 1), :, lanes_out], qs.at[c, a])
            wait_for(zout.at[a, pl.ds(0, NZ - 1), :, lanes_out], ws.at[c, a])
            wait_for(outs[a].at[pl.ds(0, NZ - 1), :, lanes_out], wr.at[c, a])
    wait_for(rs1.at[pl.ds(0, NPL - 1)], ts.at[0])
    wait_for(rs2.at[pl.ds(0, NZ - 1)], ts.at[1])
    wait_for(rs3.at[pl.ds(0, NX - 1)], ts.at[2])


def local(tq, tk, tv, tg, cq, cg, xk, xv, length):
    blocks = [a.reshape(NZ, POS // NZ, WIDTH) for a in (tq, tk, tv, tg)]
    vmem, dma = pltpu.VMEM, pltpu.SemaphoreType.DMA
    block = jax.ShapeDtypeStruct((NZ, POS // NZ, WIDTH), BF)
    oq, ok, ov, ocq, otext = pl.pallas_call(
        kernel,
        name="attend_back",
        out_shape=(
            block,
            block,
            block,
            jax.ShapeDtypeStruct((POS, WIDTH), BF),
            jax.ShapeDtypeStruct((TEXT, 128), F32),
        ),
        in_specs=[pl.BlockSpec(memory_space=vmem)] * 8 + [pl.BlockSpec(memory_space=pltpu.SMEM)],
        out_specs=[pl.BlockSpec(memory_space=vmem)] * 5,
        scratch_shapes=[
            vmem((4, NZ, 8, WIDTH), BF),
            vmem((4, NPL, NZ, WIDTH), BF),
            vmem((4, NPL, NZ, WIDTH), BF),
            vmem((3, NPL, NZ, WIDTH), BF),
            vmem((3, NPL, NZ, WIDTH), BF),
            vmem((3, NZ, 8, WIDTH), BF),
            vmem((WIDTH // 128, POS, 128), F32),
            vmem((2, TEXT, WIDTH), F32),
            vmem((NPL, 2, TEXT_ROWS, HALF), F32),
            vmem((NZ, TEXT_ROWS, 128), BF),
            vmem((NZ, TEXT_ROWS, 128), BF),
            vmem((NX, TEXT_ROWS, 128), F32),
            vmem((NX, TEXT_ROWS, 128), F32),
            dma((2, 4)),
            dma((2, 4)),
            dma((2, 4)),
            dma((2, 4)),
            dma((2, 3)),
            dma((2, 3)),
            dma((2, 3)),
            dma((2, 3)),
            dma((3,)),
            dma((3,)),
        ],
        compiler_params=pltpu.CompilerParams(collective_id=0, has_side_effects=True),
    )(*blocks, cq.reshape(POS, WIDTH), cg.reshape(POS, WIDTH), xk, xv, length)
    whole = (1, POS, WIDTH)
    return oq.reshape(whole), ok.reshape(whole), ov.reshape(whole), ocq.reshape(whole), otext[:, : HEAD_DIM // NX]


def solution(mesh):
    torus = Mesh(mesh.devices.reshape(mesh.shape["clip"], 2, NZ, NX), CLIP_SEQ)
    tokens = P(CLIP_SEQ, None, None)
    return jax.shard_map(
        local,
        mesh=torus,
        in_specs=(tokens,) * 6 + (P("clip", None), P("clip", None), P("clip")),
        out_specs=(tokens,) * 4 + (P("clip", SEQ),),
        check_vma=False,
    )
```

```python
import math

import jax
import jax.numpy as jnp
from jax import lax
from jax.experimental import pallas as pl
from jax.experimental.pallas import tpu as pltpu
from jax.sharding import Mesh
from jax.sharding import PartitionSpec as P

HEADS = 16
HEAD_DIM = 72
WIDTH = HEADS * HEAD_DIM
POS = 128
TEXT = 160
NZ = 16
NP = NZ // 2
NX = 4
NPL = 8
SCALE = 1.0 / math.sqrt(HEAD_DIM)
CLIP_SEQ = ("clip", "seq_0", "seq_1", "seq_2")
SEQ = ("seq_0", "seq_1", "seq_2")
MESH = pl.DeviceIdType.MESH
BF = jnp.bfloat16
F32 = jnp.float32

IN_CHUNKS = ((0, 640), (640, 512))
HEAD_CHUNKS = ((0, 8), (8, 16))
OUT_CHUNKS = ((0, 512), (512, 640))
DISTANCES = (8, 7, 9, 6, 10, 5, 11, 4, 12, 3, 13, 2, 14, 1, 15)
PAIR_DISTANCES = (4, 3, 5, 2, 6, 1, 7)
TEXT_ROWS = TEXT // NX
HALF = 640


def window(head):
    low = HEAD_DIM * head // 128 * 128
    return low, -(-HEAD_DIM * (head + 1) // 128) * 128


def head_mask(head):
    low, high = window(head)
    lane = lax.broadcasted_iota(jnp.int32, (1, high - low), 1) + low
    inside = (lane >= HEAD_DIM * head) & (lane < HEAD_DIM * (head + 1))
    return jnp.where(inside, 1.0, 0.0).astype(BF)


def across(a, b):
    return lax.dot_general(a, b, (((1,), (1,)), ((), ())), preferred_element_type=F32)


def down(a, b):
    return lax.dot_general(a, b, (((0,), (0,)), ((), ())), preferred_element_type=F32)


def head_back(q, k, v, g, mask, keep):
    kz, vz, qz, gz = k * mask, v * mask, q * mask, g * mask
    scores = across(kz, q) * SCALE
    if keep is not None:
        scores = jnp.where(keep, scores, -1e30)
    expo = jnp.exp(scores - jnp.max(scores, axis=0, keepdims=True))
    weights = expo * (1.0 / jnp.sum(expo, axis=0, keepdims=True))
    rounded = weights.astype(BF)
    products = across(vz, g)
    delta = jnp.sum(rounded.astype(F32) * products, axis=0, keepdims=True)
    slopes = (weights * (products - delta) * SCALE).astype(BF)
    grad_v = jnp.dot(rounded, gz, preferred_element_type=F32)
    grad_k = jnp.dot(slopes, qz, preferred_element_type=F32)
    grad_q = down(slopes, kz)
    return grad_q, grad_k, grad_v


def packed(block):
    rows = [block[8 * r : 8 * r + 8] for r in range(5)]
    last = [rows[4][:, :64], *(row[:, 64:] for row in rows), jnp.zeros((8, 24), F32)]
    parts = ([rows[0][:, :64], rows[1][:, :64]], [rows[2][:, :64], rows[3][:, :64]], last)
    return jnp.concatenate([jnp.concatenate(part, axis=1) for part in parts], axis=0)


def unpacked(block):
    rows = [block[8 * (r // 2) : 8 * (r // 2) + 8, 64 * (r % 2) : 64 * (r % 2) + 64] for r in range(5)]
    rest = [block[16:24, 64 + 8 * r : 72 + 8 * r] for r in range(5)]
    return jnp.concatenate([jnp.concatenate(pair, axis=1) for pair in zip(rows, rest, strict=True)], axis=0)


class Tiles:
    def __init__(self, store):
        self.open, self.store = {}, store

    def add(self, head, value):
        low, high = window(head)
        for t in range(low // 128, high // 128):
            part = value[:, 128 * t - low : 128 * t - low + 128]
            self.open[t] = part if t not in self.open else self.open[t] + part
            if HEAD_DIM * (head + 1) >= 128 * (t + 1):
                self.store(t, self.open.pop(t))


def kernel(
    tq, tk, tv, tg, cq, cg, xk, xv, length,
    oq, ok, ov, ocq, otext,
    zbuf, pout, pbuf, gbuf, qbuf, zout, tall, tpart, rs1, rsout, rsmine, rsin, rs2out, rs2, rs3out, rs3, cqb, cgb, xkb, xvb,
    zs, zr, ps, pr, qs, qr, ws, wr, ts, tr, ls, os,
):
    y, z, x = lax.axis_index("seq_0"), lax.axis_index("seq_1"), lax.axis_index("seq_2")
    me = y * NX + x
    parity, pair = lax.rem(z, 2), z // 2
    turned = lax.rem(z + lax.rem(lax.axis_index("clip"), 2), 2)
    partner = lax.rem(z + 1 - 2 * turned + NZ, NZ)
    ins, outs = (tq, tk, tv, tg), (oq, ok, ov)

    def z_peer(k):
        return lax.rem(z + k, NZ)

    def plane_peer(k):
        return lax.rem(y + k // NX, 2), lax.rem(x + k % NX, NX)

    def in_plane(k):
        py, px = plane_peer(k)
        return {"seq_0": py, "seq_2": px}

    barrier = pltpu.get_barrier_semaphore()
    for k in range(1, NZ):
        pl.semaphore_signal(barrier, 1, device_id={"seq_1": z_peer(k)}, device_id_type=MESH)
    for k in range(1, NPL):
        pl.semaphore_signal(barrier, 1, device_id=in_plane(k), device_id_type=MESH)
    loads = [pltpu.make_async_copy(*pair, ls.at[i]) for i, pair in enumerate(((cq, cqb), (cg, cgb), (xk, xkb), (xv, xvb)))]
    loads += [pltpu.make_async_copy(ins[a].at[z], zbuf.at[a, z], ls.at[4 + a]) for a in range(4)]
    for copy in loads:
        copy.start()
    pl.semaphore_wait(barrier, NZ - 1 + NPL - 1)

    def send(src, dst, send_sem, recv_sem, device):
        pltpu.make_async_remote_copy(
            src_ref=src, dst_ref=dst, send_sem=send_sem, recv_sem=recv_sem, device_id=device, device_id_type=MESH
        ).start()

    def wait_for(ref, sem):
        pltpu.make_async_copy(ref, ref, sem).wait()

    for c, (low, size) in enumerate(IN_CHUNKS):
        lanes = pl.ds(low, size)
        for a in range(4):
            for k in DISTANCES:
                peer = z_peer(k)
                send(ins[a].at[peer, :, lanes], zbuf.at[a, z, :, lanes], zs.at[c, a], zr.at[c, a], {"seq_1": peer})
    for copy in loads:
        copy.wait()

    text_rows = lax.broadcasted_iota(jnp.int32, (TEXT, POS), 0)
    keep = text_rows < length[0]

    def put_cross(t, value):
        ocq[:, 128 * t : 128 * t + 128] = value.astype(BF)

    def put_text(kind):
        def put(t, value):
            tpart[kind, :, 128 * t : 128 * t + 128] = value

        return put

    sums = (Tiles(put_cross), Tiles(put_text(0)), Tiles(put_text(1)))
    for h in range(HEADS):
        low, high = window(h)
        grads = head_back(*(b[:, low:high] for b in (cqb, xkb, xvb, cgb)), head_mask(h), keep)
        for s, grad in zip(sums, grads, strict=True):
            s.add(h, grad)

    for k in range(1, NPL):
        py, px = plane_peer(k)
        rows, lanes = pl.ds(pl.multiple_of(px * TEXT_ROWS, 8), TEXT_ROWS), pl.ds(pl.multiple_of(py * 512, 128), HALF)
        send(tpart.at[:, rows, lanes], rs1.at[me], ts.at[0], tr.at[0], in_plane(k))
    own_rows, own_lanes = pl.ds(pl.multiple_of(x * TEXT_ROWS, 8), TEXT_ROWS), pl.ds(pl.multiple_of(y * 512, 128), HALF)
    rs1[me] = tpart[:, own_rows, own_lanes]

    def hand_on(c):
        low, size = IN_CHUNKS[c]
        lanes = pl.ds(low, size)
        for a in range(4):
            wait_for(zbuf.at[a, pl.ds(0, NZ - 1), :, lanes], zr.at[c, a])
            for t in range(low, low + size, 128):
                for f in range(NZ):
                    tall[t // 128, pl.ds(f, NPL, stride=NZ), :] = zbuf[a, f, :, t : t + 128].astype(F32)
                for j in range(NPL):
                    pout[a, j, :, t : t + 128] = tall[t // 128, NZ * j : NZ * j + NZ, :].astype(BF)
            for k in range(1, NPL):
                py, px = plane_peer(k)
                send(pout.at[a, py * NX + px, :, lanes], pbuf.at[a, me, :, lanes], ps.at[c, a], pr.at[c, a], in_plane(k))
            pbuf[a, me, :, low : low + size] = pout[a, me, :, low : low + size]

    def put_temporal(a):
        def put(t, value):
            gbuf[a, :, :, 128 * t : 128 * t + 128] = value.astype(BF).reshape(NPL, NZ, 128)

        return put

    temporal = tuple(Tiles(put_temporal(a)) for a in range(3))

    def attend(c):
        low, size = IN_CHUNKS[c]
        for a in range(4):
            wait_for(pbuf.at[a, pl.ds(0, NPL - 1), :, pl.ds(low, size)], pr.at[c, a])
        for h in range(*HEAD_CHUNKS[c]):
            lo, hi = window(h)
            q, k, v, g = (pbuf[a, :, :, lo:hi].reshape(POS, hi - lo) for a in range(4))
            for s, grad in zip(temporal, head_back(q, k, v, g, head_mask(h), None), strict=True):
                s.add(h, grad)

    def give_back(c):
        low, size = OUT_CHUNKS[c]
        lanes = pl.ds(low, size)
        for a in range(3):
            for k in range(1, NPL):
                py, px = plane_peer(k)
                send(gbuf.at[a, py * NX + px, :, lanes], qbuf.at[a, me, :, lanes], qs.at[c, a], qr.at[c, a], in_plane(k))
            qbuf[a, me, :, low : low + size] = gbuf[a, me, :, low : low + size]

    def deliver(c):
        low, size = OUT_CHUNKS[c]
        lanes = pl.ds(low, size)
        for a in range(3):
            wait_for(qbuf.at[a, pl.ds(0, NPL - 1), :, lanes], qr.at[c, a])
            for t in range(low, low + size, 128):
                for j in range(NPL):
                    tall[t // 128, pl.ds(j, NZ, stride=NPL), :] = qbuf[a, j, :, t : t + 128].astype(F32)
                for f in range(NZ):
                    zout[a, f, :, t : t + 128] = tall[t // 128, NPL * f : NPL * f + NPL, :].astype(BF)
            for k in DISTANCES:
                peer = z_peer(k)
                send(zout.at[a, peer, :, lanes], outs[a].at[z, :, lanes], ws.at[c, a], wr.at[c, a], {"seq_1": peer})
            pltpu.make_async_copy(zout.at[a, z, :, lanes], outs[a].at[z, :, lanes], os.at[c, a]).start()

    hand_on(0)

    wait_for(rs1.at[pl.ds(0, NPL - 1)], tr.at[0])
    keys, values = (sum((rs1[j, kind] for j in range(1, NPL)), rs1[0, kind]) for kind in range(2))
    rsmine[...] = jnp.where(parity == 0, keys, values)
    rsout[...] = jnp.where(parity == 0, values, keys).astype(BF)
    send(rsout, rsin, ts.at[1], tr.at[1], {"seq_1": partner})

    attend(0)
    give_back(0)
    deliver(0)
    hand_on(1)

    wait_for(rsin, tr.at[1])
    rsmine[...] = rsmine[...] + rsin[...].astype(F32)
    for i in range(NP):
        first, second = (rsmine[:, s : s + HEAD_DIM] for s in (HEAD_DIM * i, HEAD_DIM * i + 64))
        rs2out[i] = packed(jnp.where(y == 0, first, second)).astype(BF)
    for k in PAIR_DISTANCES:
        peer = lax.rem(pair + k, NP)
        send(rs2out.at[peer], rs2.at[pair], ts.at[2], tr.at[2], {"seq_1": 2 * peer + parity})
    rs2[pair] = rs2out[pair]

    attend(1)
    give_back(1)
    deliver(1)

    wait_for(rs2.at[pl.ds(0, NP - 1)], tr.at[2])
    total = unpacked(sum((rs2[f].astype(F32) for f in range(1, NP)), rs2[0].astype(F32)))
    columns = HEAD_DIM // NX
    for j in range(NX):
        rs3out[j] = jnp.pad(total[:, columns * j : columns * j + columns], ((0, 0), (0, 128 - columns)))
    for k in range(1, NX):
        _, px = plane_peer(k)
        send(rs3out.at[px], rs3.at[x], ts.at[3], tr.at[3], in_plane(k))
    rs3[x] = rs3out[x]

    wait_for(rs3.at[pl.ds(0, NX - 1)], tr.at[3])
    otext[...] = jnp.transpose(rs3[...].reshape(TEXT, 128))[:columns, :]

    for c in range(2):
        lanes_in, lanes_out = pl.ds(*IN_CHUNKS[c]), pl.ds(*OUT_CHUNKS[c])
        for a in range(4):
            wait_for(zbuf.at[a, pl.ds(0, NZ - 1), :, lanes_in], zs.at[c, a])
            wait_for(pout.at[a, pl.ds(0, NPL - 1), :, lanes_in], ps.at[c, a])
        for a in range(3):
            wait_for(gbuf.at[a, pl.ds(0, NPL - 1), :, lanes_out], qs.at[c, a])
            wait_for(zout.at[a, pl.ds(0, NZ - 1), :, lanes_out], ws.at[c, a])
            wait_for(outs[a].at[pl.ds(0, NZ - 1), :, lanes_out], wr.at[c, a])
            wait_for(outs[a].at[0, :, lanes_out], os.at[c, a])
    wait_for(rs1.at[pl.ds(0, NPL - 1)], ts.at[0])
    wait_for(rsin, ts.at[1])
    wait_for(rs2.at[pl.ds(0, NP - 1)], ts.at[2])
    wait_for(rs3.at[pl.ds(0, NX - 1)], ts.at[3])


def move(count, *refs):
    copies = [pltpu.make_async_copy(refs[i], refs[count + i], refs[2 * count].at[i]) for i in range(count)]
    for copy in copies:
        copy.start()
    for copy in copies:
        copy.wait()


def local(tq, tk, tv, tg, cq, cg, xk, xv, length):
    arrays = [a.reshape(NZ, POS // NZ, WIDTH) for a in (tq, tk, tv, tg)]
    arrays += [cq.reshape(POS, WIDTH), cg.reshape(POS, WIDTH), xk, xv]
    vmem, dma = pltpu.VMEM, pltpu.SemaphoreType.DMA
    anywhere = pl.BlockSpec(memory_space=pl.ANY)
    block = jax.ShapeDtypeStruct((NZ, POS // NZ, WIDTH), BF)
    shapes = (
        block,
        block,
        block,
        jax.ShapeDtypeStruct((POS, WIDTH), BF),
        jax.ShapeDtypeStruct((HEAD_DIM // NX, TEXT), F32),
    )
    grads = pl.pallas_call(
        kernel,
        name="attend_back",
        out_shape=shapes,
        in_specs=[pl.BlockSpec(memory_space=pltpu.HBM)] * 8 + [pl.BlockSpec(memory_space=pltpu.SMEM)],
        out_specs=[anywhere] * 3 + [pl.BlockSpec(memory_space=vmem)] * 2,
        scratch_shapes=[
            vmem((4, NZ, 8, WIDTH), BF),
            vmem((4, NPL, NZ, WIDTH), BF),
            vmem((4, NPL, NZ, WIDTH), BF),
            vmem((3, NPL, NZ, WIDTH), BF),
            vmem((3, NPL, NZ, WIDTH), BF),
            vmem((3, NZ, 8, WIDTH), BF),
            vmem((WIDTH // 128, POS, 128), F32),
            vmem((2, TEXT, WIDTH), F32),
            vmem((NPL, 2, TEXT_ROWS, HALF), F32),
            vmem((TEXT_ROWS, HALF), BF),
            vmem((TEXT_ROWS, HALF), F32),
            vmem((TEXT_ROWS, HALF), BF),
            vmem((NP, 24, 128), BF),
            vmem((NP, 24, 128), BF),
            vmem((NX, TEXT_ROWS, 128), F32),
            vmem((NX, TEXT_ROWS, 128), F32),
            vmem((POS, WIDTH), BF),
            vmem((POS, WIDTH), BF),
            vmem((TEXT, WIDTH), BF),
            vmem((TEXT, WIDTH), BF),
            dma((2, 4)),
            dma((2, 4)),
            dma((2, 4)),
            dma((2, 4)),
            dma((2, 3)),
            dma((2, 3)),
            dma((2, 3)),
            dma((2, 3)),
            dma((4,)),
            dma((4,)),
            dma((8,)),
            dma((2, 3)),
        ],
        compiler_params=pltpu.CompilerParams(
            collective_id=0, has_side_effects=True, vmem_limit_bytes=32 * 2**20
        ),
    )(*(pltpu.with_memory_space_constraint(a, pltpu.HBM) for a in arrays), length)
    count = len(shapes)
    oq, ok, ov, ocq, otext = pl.pallas_call(
        lambda *refs: move(count, *refs),
        name="move",
        out_shape=shapes,
        in_specs=[anywhere] * count,
        out_specs=[anywhere] * count,
        scratch_shapes=[dma((count,))],
        compiler_params=pltpu.CompilerParams(vmem_limit_bytes=2**20),
    )(*grads)
    whole = (1, POS, WIDTH)
    return oq.reshape(whole), ok.reshape(whole), ov.reshape(whole), ocq.reshape(whole), otext.T


def solution(mesh):
    torus = Mesh(mesh.devices.reshape(mesh.shape["clip"], 2, NZ, NX), CLIP_SEQ)
    tokens = P(CLIP_SEQ, None, None)
    return jax.shard_map(
        local,
        mesh=torus,
        in_specs=(tokens,) * 6 + (P("clip", None), P("clip", None), P("clip")),
        out_specs=(tokens,) * 4 + (P("clip", SEQ),),
        check_vma=False,
    )
```

```python
import math

import jax
import jax.numpy as jnp
from jax import lax
from jax.experimental import pallas as pl
from jax.experimental.pallas import tpu as pltpu
from jax.sharding import Mesh
from jax.sharding import PartitionSpec as P

HEADS = 16
HEAD_DIM = 72
WIDTH = HEADS * HEAD_DIM
POS = 128
TEXT = 160
NZ = 16
NP = NZ // 2
NX = 4
NPL = 8
SCALE = 1.0 / math.sqrt(HEAD_DIM)
CLIP_SEQ = ("clip", "seq_0", "seq_1", "seq_2")
SEQ = ("seq_0", "seq_1", "seq_2")
MESH = pl.DeviceIdType.MESH
BF = jnp.bfloat16
F32 = jnp.float32

IN_CHUNKS = ((0, 640), (640, 512))
HEAD_CHUNKS = ((0, 8), (8, 16))
OUT_CHUNKS = ((0, 512), (512, 640))
DISTANCES = (8, 7, 9, 6, 10, 5, 11, 4, 12, 3, 13, 2, 14, 1, 15)
PAIR_DISTANCES = (4, 3, 5, 2, 6, 1, 7)
TEXT_ROWS = TEXT // NX
HALF = 640


def window(head):
    low = HEAD_DIM * head // 128 * 128
    return low, -(-HEAD_DIM * (head + 1) // 128) * 128


def head_mask(head):
    low, high = window(head)
    lane = lax.broadcasted_iota(jnp.int32, (1, high - low), 1) + low
    inside = (lane >= HEAD_DIM * head) & (lane < HEAD_DIM * (head + 1))
    return jnp.where(inside, 1.0, 0.0).astype(BF)


def across(a, b):
    return lax.dot_general(a, b, (((1,), (1,)), ((), ())), preferred_element_type=F32)


def down(a, b):
    return lax.dot_general(a, b, (((0,), (0,)), ((), ())), preferred_element_type=F32)


def head_back(q, k, v, g, mask, keep):
    kz, vz, qz, gz = k * mask, v * mask, q * mask, g * mask
    scores = across(kz, q) * SCALE
    if keep is not None:
        scores = jnp.where(keep, scores, -1e30)
    expo = jnp.exp(scores - jnp.max(scores, axis=0, keepdims=True))
    weights = expo * (1.0 / jnp.sum(expo, axis=0, keepdims=True))
    rounded = weights.astype(BF)
    products = across(vz, g)
    delta = jnp.sum(rounded.astype(F32) * products, axis=0, keepdims=True)
    slopes = (weights * (products - delta) * SCALE).astype(BF)
    grad_v = jnp.dot(rounded, gz, preferred_element_type=F32)
    grad_k = jnp.dot(slopes, qz, preferred_element_type=F32)
    grad_q = down(slopes, kz)
    return grad_q, grad_k, grad_v


def packed(block):
    rows = [block[8 * r : 8 * r + 8] for r in range(5)]
    last = [rows[4][:, :64], *(row[:, 64:] for row in rows), jnp.zeros((8, 24), F32)]
    parts = ([rows[0][:, :64], rows[1][:, :64]], [rows[2][:, :64], rows[3][:, :64]], last)
    return jnp.concatenate([jnp.concatenate(part, axis=1) for part in parts], axis=0)


def unpacked(block):
    rows = [block[8 * (r // 2) : 8 * (r // 2) + 8, 64 * (r % 2) : 64 * (r % 2) + 64] for r in range(5)]
    rest = [block[16:24, 64 + 8 * r : 72 + 8 * r] for r in range(5)]
    return jnp.concatenate([jnp.concatenate(pair, axis=1) for pair in zip(rows, rest, strict=True)], axis=0)


class Tiles:
    def __init__(self, store):
        self.open, self.store = {}, store

    def add(self, head, value):
        low, high = window(head)
        for t in range(low // 128, high // 128):
            part = value[:, 128 * t - low : 128 * t - low + 128]
            self.open[t] = part if t not in self.open else self.open[t] + part
            if HEAD_DIM * (head + 1) >= 128 * (t + 1):
                self.store(t, self.open.pop(t))


def kernel(
    tq, tk, tv, tg, cq, cg, xk, xv, length,
    oq, ok, ov, ocq, otext,
    zbuf, pout, pbuf, gbuf, qbuf, zout, tall, tpart, rs1, rsout, rsmine, rsin, rs2out, rs2, rs3out, rs3, cqb, cgb, xkb, xvb, vin,
    zs, zr, ps, pr, qs, qr, ws, wr, ts, tr, ls, os, known,
):
    y, z, x = lax.axis_index("seq_0"), lax.axis_index("seq_1"), lax.axis_index("seq_2")
    me = y * NX + x
    parity, pair = lax.rem(z, 2), z // 2
    turned = lax.rem(z + lax.rem(lax.axis_index("clip"), 2), 2)
    partner = lax.rem(z + 1 - 2 * turned + NZ, NZ)
    ins, outs = (tq, tk, tv, tg), (oq, ok, ov)

    def z_peer(k):
        return lax.rem(z + k, NZ)

    def plane_peer(k):
        return lax.rem(y + k // NX, 2), lax.rem(x + k % NX, NX)

    def in_plane(k):
        py, px = plane_peer(k)
        return {"seq_0": py, "seq_2": px}

    def at_z(k):
        return {"seq_1": z_peer(k % NZ)}

    barrier = pltpu.get_barrier_semaphore()
    near = [at_z(k) for k in (1, -1, 2, -2)] + [in_plane(k) for k in (1, 3, 4)]
    for device in near:
        pl.semaphore_signal(barrier, 1, device_id=device, device_id_type=MESH)

    def send(src, dst, send_sem, recv_sem, device):
        pltpu.make_async_remote_copy(
            src_ref=src, dst_ref=dst, send_sem=send_sem, recv_sem=recv_sem, device_id=device, device_id_type=MESH
        ).start()

    def wait_for(ref, sem):
        pltpu.make_async_copy(ref, ref, sem).wait()

    own = [pltpu.make_async_copy(ins[a], vin.at[a], ls.at[a]) for a in range(4)]
    cross = [pltpu.make_async_copy(*pair, ls.at[4 + i]) for i, pair in enumerate(((cq, cqb), (cg, cgb), (xk, xkb), (xv, xvb)))]
    for copy in own + cross:
        copy.start()
    for copy in own:
        copy.wait()

    def spread(c, distances):
        lanes = pl.ds(*IN_CHUNKS[c])
        for a in range(4):
            for k in distances:
                peer = z_peer(k % NZ)
                send(vin.at[a, peer, :, lanes], zbuf.at[a, z, :, lanes], zs.at[c, a], zr.at[c, a], {"seq_1": peer})

    def pass_on(i, devices):
        for device in devices:
            pl.semaphore_signal(known.at[i], 1, device_id=device, device_id_type=MESH)

    pl.semaphore_wait(barrier, len(near))
    pass_on(0, (at_z(2), at_z(-2)))
    spread(0, (2, -2, 1, -1))
    pl.semaphore_wait(known.at[0], 2)
    pass_on(1, (at_z(4), at_z(-4)))
    pass_on(2, [in_plane(k) for k in (1, 3, 4)])
    spread(0, (4, -4, 3, -3))
    pl.semaphore_wait(known.at[1], 2)
    spread(0, (8, 7, -7, 6, -6, 5, -5))
    spread(1, DISTANCES)
    for a in range(4):
        zbuf[a, z] = vin[a, z]
    for copy in cross:
        copy.wait()

    text_rows = lax.broadcasted_iota(jnp.int32, (TEXT, POS), 0)
    keep = text_rows < length[0]

    def put_cross(t, value):
        ocq[:, 128 * t : 128 * t + 128] = value.astype(BF)

    def put_text(kind):
        def put(t, value):
            tpart[kind, :, 128 * t : 128 * t + 128] = value

        return put

    sums = (Tiles(put_cross), Tiles(put_text(0)), Tiles(put_text(1)))
    for h in range(HEADS):
        low, high = window(h)
        grads = head_back(*(b[:, low:high] for b in (cqb, xkb, xvb, cgb)), head_mask(h), keep)
        for s, grad in zip(sums, grads, strict=True):
            s.add(h, grad)

    pl.semaphore_wait(known.at[2], 3)
    pass_on(3, (in_plane(4),))
    pl.semaphore_wait(known.at[3], 1)

    for k in range(1, NPL):
        py, px = plane_peer(k)
        rows, lanes = pl.ds(pl.multiple_of(px * TEXT_ROWS, 8), TEXT_ROWS), pl.ds(pl.multiple_of(py * 512, 128), HALF)
        send(tpart.at[:, rows, lanes], rs1.at[me], ts.at[0], tr.at[0], in_plane(k))
    own_rows, own_lanes = pl.ds(pl.multiple_of(x * TEXT_ROWS, 8), TEXT_ROWS), pl.ds(pl.multiple_of(y * 512, 128), HALF)
    rs1[me] = tpart[:, own_rows, own_lanes]

    def hand_on(c):
        low, size = IN_CHUNKS[c]
        lanes = pl.ds(low, size)
        for a in range(4):
            wait_for(zbuf.at[a, pl.ds(0, NZ - 1), :, lanes], zr.at[c, a])
            for t in range(low, low + size, 128):
                for f in range(NZ):
                    tall[t // 128, pl.ds(f, NPL, stride=NZ), :] = zbuf[a, f, :, t : t + 128].astype(F32)
                for j in range(NPL):
                    pout[a, j, :, t : t + 128] = tall[t // 128, NZ * j : NZ * j + NZ, :].astype(BF)
            for k in range(1, NPL):
                py, px = plane_peer(k)
                send(pout.at[a, py * NX + px, :, lanes], pbuf.at[a, me, :, lanes], ps.at[c, a], pr.at[c, a], in_plane(k))
            pbuf[a, me, :, low : low + size] = pout[a, me, :, low : low + size]

    def put_temporal(a):
        def put(t, value):
            gbuf[a, :, :, 128 * t : 128 * t + 128] = value.astype(BF).reshape(NPL, NZ, 128)

        return put

    temporal = tuple(Tiles(put_temporal(a)) for a in range(3))

    def attend(c):
        low, size = IN_CHUNKS[c]
        for a in range(4):
            wait_for(pbuf.at[a, pl.ds(0, NPL - 1), :, pl.ds(low, size)], pr.at[c, a])
        for h in range(*HEAD_CHUNKS[c]):
            lo, hi = window(h)
            q, k, v, g = (pbuf[a, :, :, lo:hi].reshape(POS, hi - lo) for a in range(4))
            for s, grad in zip(temporal, head_back(q, k, v, g, head_mask(h), None), strict=True):
                s.add(h, grad)

    def give_back(c):
        low, size = OUT_CHUNKS[c]
        lanes = pl.ds(low, size)
        for a in range(3):
            for k in range(1, NPL):
                py, px = plane_peer(k)
                send(gbuf.at[a, py * NX + px, :, lanes], qbuf.at[a, me, :, lanes], qs.at[c, a], qr.at[c, a], in_plane(k))
            qbuf[a, me, :, low : low + size] = gbuf[a, me, :, low : low + size]

    def deliver(c):
        low, size = OUT_CHUNKS[c]
        lanes = pl.ds(low, size)
        for a in range(3):
            wait_for(qbuf.at[a, pl.ds(0, NPL - 1), :, lanes], qr.at[c, a])
            for t in range(low, low + size, 128):
                for j in range(NPL):
                    tall[t // 128, pl.ds(j, NZ, stride=NPL), :] = qbuf[a, j, :, t : t + 128].astype(F32)
                for f in range(NZ):
                    zout[a, f, :, t : t + 128] = tall[t // 128, NPL * f : NPL * f + NPL, :].astype(BF)
            for k in DISTANCES:
                peer = z_peer(k)
                send(zout.at[a, peer, :, lanes], outs[a].at[z, :, lanes], ws.at[c, a], wr.at[c, a], {"seq_1": peer})
            pltpu.make_async_copy(zout.at[a, z, :, lanes], outs[a].at[z, :, lanes], os.at[c, a]).start()

    hand_on(0)

    wait_for(rs1.at[pl.ds(0, NPL - 1)], tr.at[0])
    keys, values = (sum((rs1[j, kind] for j in range(1, NPL)), rs1[0, kind]) for kind in range(2))
    rsmine[...] = jnp.where(parity == 0, keys, values)
    rsout[...] = jnp.where(parity == 0, values, keys).astype(BF)
    send(rsout, rsin, ts.at[1], tr.at[1], {"seq_1": partner})

    attend(0)
    give_back(0)
    deliver(0)
    hand_on(1)

    wait_for(rsin, tr.at[1])
    rsmine[...] = rsmine[...] + rsin[...].astype(F32)
    for i in range(NP):
        first, second = (rsmine[:, s : s + HEAD_DIM] for s in (HEAD_DIM * i, HEAD_DIM * i + 64))
        rs2out[i] = packed(jnp.where(y == 0, first, second)).astype(BF)
    for k in PAIR_DISTANCES:
        peer = lax.rem(pair + k, NP)
        send(rs2out.at[peer], rs2.at[pair], ts.at[2], tr.at[2], {"seq_1": 2 * peer + parity})
    rs2[pair] = rs2out[pair]

    attend(1)
    give_back(1)
    deliver(1)

    wait_for(rs2.at[pl.ds(0, NP - 1)], tr.at[2])
    total = unpacked(sum((rs2[f].astype(F32) for f in range(1, NP)), rs2[0].astype(F32)))
    columns = HEAD_DIM // NX
    for j in range(NX):
        rs3out[j] = jnp.pad(total[:, columns * j : columns * j + columns], ((0, 0), (0, 128 - columns)))
    for k in range(1, NX):
        _, px = plane_peer(k)
        send(rs3out.at[px], rs3.at[x], ts.at[3], tr.at[3], in_plane(k))
    rs3[x] = rs3out[x]

    wait_for(rs3.at[pl.ds(0, NX - 1)], tr.at[3])
    otext[...] = jnp.transpose(rs3[...].reshape(TEXT, 128))[:columns, :]

    for c in range(2):
        lanes_in, lanes_out = pl.ds(*IN_CHUNKS[c]), pl.ds(*OUT_CHUNKS[c])
        for a in range(4):
            wait_for(zbuf.at[a, pl.ds(0, NZ - 1), :, lanes_in], zs.at[c, a])
            wait_for(pout.at[a, pl.ds(0, NPL - 1), :, lanes_in], ps.at[c, a])
        for a in range(3):
            wait_for(gbuf.at[a, pl.ds(0, NPL - 1), :, lanes_out], qs.at[c, a])
            wait_for(zout.at[a, pl.ds(0, NZ - 1), :, lanes_out], ws.at[c, a])
            wait_for(outs[a].at[pl.ds(0, NZ - 1), :, lanes_out], wr.at[c, a])
            wait_for(outs[a].at[0, :, lanes_out], os.at[c, a])
    wait_for(rs1.at[pl.ds(0, NPL - 1)], ts.at[0])
    wait_for(rsin, ts.at[1])
    wait_for(rs2.at[pl.ds(0, NP - 1)], ts.at[2])
    wait_for(rs3.at[pl.ds(0, NX - 1)], ts.at[3])


def move(count, *refs):
    copies = [pltpu.make_async_copy(refs[i], refs[count + i], refs[2 * count].at[i]) for i in range(count)]
    for copy in copies:
        copy.start()
    for copy in copies:
        copy.wait()


def local(tq, tk, tv, tg, cq, cg, xk, xv, length):
    arrays = [a.reshape(NZ, POS // NZ, WIDTH) for a in (tq, tk, tv, tg)]
    arrays += [cq.reshape(POS, WIDTH), cg.reshape(POS, WIDTH), xk, xv]
    vmem, dma = pltpu.VMEM, pltpu.SemaphoreType.DMA
    anywhere = pl.BlockSpec(memory_space=pl.ANY)
    block = jax.ShapeDtypeStruct((NZ, POS // NZ, WIDTH), BF)
    shapes = (
        block,
        block,
        block,
        jax.ShapeDtypeStruct((POS, WIDTH), BF),
        jax.ShapeDtypeStruct((HEAD_DIM // NX, TEXT), F32),
    )
    grads = pl.pallas_call(
        kernel,
        name="attend_back",
        out_shape=shapes,
        in_specs=[pl.BlockSpec(memory_space=pltpu.HBM)] * 8 + [pl.BlockSpec(memory_space=pltpu.SMEM)],
        out_specs=[anywhere] * 3 + [pl.BlockSpec(memory_space=vmem)] * 2,
        scratch_shapes=[
            vmem((4, NZ, 8, WIDTH), BF),
            vmem((4, NPL, NZ, WIDTH), BF),
            vmem((4, NPL, NZ, WIDTH), BF),
            vmem((3, NPL, NZ, WIDTH), BF),
            vmem((3, NPL, NZ, WIDTH), BF),
            vmem((3, NZ, 8, WIDTH), BF),
            vmem((WIDTH // 128, POS, 128), F32),
            vmem((2, TEXT, WIDTH), F32),
            vmem((NPL, 2, TEXT_ROWS, HALF), F32),
            vmem((TEXT_ROWS, HALF), BF),
            vmem((TEXT_ROWS, HALF), F32),
            vmem((TEXT_ROWS, HALF), BF),
            vmem((NP, 24, 128), BF),
            vmem((NP, 24, 128), BF),
            vmem((NX, TEXT_ROWS, 128), F32),
            vmem((NX, TEXT_ROWS, 128), F32),
            vmem((POS, WIDTH), BF),
            vmem((POS, WIDTH), BF),
            vmem((TEXT, WIDTH), BF),
            vmem((TEXT, WIDTH), BF),
            vmem((4, NZ, 8, WIDTH), BF),
            dma((2, 4)),
            dma((2, 4)),
            dma((2, 4)),
            dma((2, 4)),
            dma((2, 3)),
            dma((2, 3)),
            dma((2, 3)),
            dma((2, 3)),
            dma((4,)),
            dma((4,)),
            dma((8,)),
            dma((2, 3)),
            pltpu.SemaphoreType.REGULAR((4,)),
        ],
        compiler_params=pltpu.CompilerParams(
            collective_id=0, has_side_effects=True, vmem_limit_bytes=32 * 2**20
        ),
    )(*(pltpu.with_memory_space_constraint(a, pltpu.HBM) for a in arrays), length)
    count = len(shapes)
    oq, ok, ov, ocq, otext = pl.pallas_call(
        lambda *refs: move(count, *refs),
        name="move",
        out_shape=shapes,
        in_specs=[anywhere] * count,
        out_specs=[anywhere] * count,
        scratch_shapes=[dma((count,))],
        compiler_params=pltpu.CompilerParams(vmem_limit_bytes=2**20),
    )(*grads)
    whole = (1, POS, WIDTH)
    return oq.reshape(whole), ok.reshape(whole), ov.reshape(whole), ocq.reshape(whole), otext.T


def solution(mesh):
    torus = Mesh(mesh.devices.reshape(mesh.shape["clip"], 2, NZ, NX), CLIP_SEQ)
    tokens = P(CLIP_SEQ, None, None)
    return jax.shard_map(
        local,
        mesh=torus,
        in_specs=(tokens,) * 6 + (P("clip", None), P("clip", None), P("clip")),
        out_specs=(tokens,) * 4 + (P("clip", SEQ),),
        check_vma=False,
    )
```

```python
import math

import jax
import jax.numpy as jnp
from jax import lax
from jax.experimental import pallas as pl
from jax.experimental.pallas import tpu as pltpu
from jax.sharding import Mesh
from jax.sharding import PartitionSpec as P

HEADS = 16
HEAD_DIM = 72
WIDTH = HEADS * HEAD_DIM
POS = 128
TEXT = 160
NZ = 16
NP = NZ // 2
NX = 4
NPL = 8
SCALE = 1.0 / math.sqrt(HEAD_DIM)
CLIP_SEQ = ("clip", "seq_0", "seq_1", "seq_2")
SEQ = ("seq_0", "seq_1", "seq_2")
MESH = pl.DeviceIdType.MESH
BF = jnp.bfloat16
F32 = jnp.float32

IN_CHUNKS = ((0, 640), (640, 512))
HEAD_CHUNKS = ((0, 8), (8, 16))
OUT_CHUNKS = ((0, 512), (512, 640))
DISTANCES = (8, 7, 9, 6, 10, 5, 11, 4, 12, 3, 13, 2, 14, 1, 15)
PAIR_DISTANCES = (4, 3, 5, 2, 6, 1, 7)
TEXT_ROWS = TEXT // NX
HALF = 640


def window(head):
    low = HEAD_DIM * head // 128 * 128
    return low, -(-HEAD_DIM * (head + 1) // 128) * 128


def head_mask(head):
    low, high = window(head)
    lane = lax.broadcasted_iota(jnp.int32, (1, high - low), 1) + low
    inside = (lane >= HEAD_DIM * head) & (lane < HEAD_DIM * (head + 1))
    return jnp.where(inside, 1.0, 0.0).astype(BF)


def across(a, b):
    return lax.dot_general(a, b, (((1,), (1,)), ((), ())), preferred_element_type=F32)


def down(a, b):
    return lax.dot_general(a, b, (((0,), (0,)), ((), ())), preferred_element_type=F32)


def head_back(q, k, v, g, mask, keep):
    kz, vz, qz, gz = k * mask, v * mask, q * mask, g * mask
    scores = across(kz, q) * SCALE
    if keep is not None:
        scores = jnp.where(keep, scores, -1e30)
    expo = jnp.exp(scores - jnp.max(scores, axis=0, keepdims=True))
    weights = expo * (1.0 / jnp.sum(expo, axis=0, keepdims=True))
    rounded = weights.astype(BF)
    products = across(vz, g)
    delta = jnp.sum(rounded.astype(F32) * products, axis=0, keepdims=True)
    slopes = (weights * (products - delta) * SCALE).astype(BF)
    grad_v = jnp.dot(rounded, gz, preferred_element_type=F32)
    grad_k = jnp.dot(slopes, qz, preferred_element_type=F32)
    grad_q = down(slopes, kz)
    return grad_q, grad_k, grad_v


def packed(block):
    rows = [block[8 * r : 8 * r + 8] for r in range(5)]
    last = [rows[4][:, :64], *(row[:, 64:] for row in rows), jnp.zeros((8, 24), F32)]
    parts = ([rows[0][:, :64], rows[1][:, :64]], [rows[2][:, :64], rows[3][:, :64]], last)
    return jnp.concatenate([jnp.concatenate(part, axis=1) for part in parts], axis=0)


def unpacked(block):
    rows = [block[8 * (r // 2) : 8 * (r // 2) + 8, 64 * (r % 2) : 64 * (r % 2) + 64] for r in range(5)]
    rest = [block[16:24, 64 + 8 * r : 72 + 8 * r] for r in range(5)]
    return jnp.concatenate([jnp.concatenate(pair, axis=1) for pair in zip(rows, rest, strict=True)], axis=0)


class Tiles:
    def __init__(self, store):
        self.open, self.store = {}, store

    def add(self, head, value):
        low, high = window(head)
        for t in range(low // 128, high // 128):
            part = value[:, 128 * t - low : 128 * t - low + 128]
            self.open[t] = part if t not in self.open else self.open[t] + part
            if HEAD_DIM * (head + 1) >= 128 * (t + 1):
                self.store(t, self.open.pop(t))


def kernel(
    tq, tk, tv, tg, cq, cg, xk, xv, length,
    oq, ok, ov, ocq, otext,
    zbuf, pout, pbuf, gbuf, qbuf, zout, tall, tpart, rs1, rsout, rsmine, rsin, rs2out, rs2, rs3out, rs3, cqb, cgb, xkb, xvb, vin,
    zs, zr, ps, pr, qs, qr, ws, wr, ts, tr, ls, os, known,
):
    y, z, x = lax.axis_index("seq_0"), lax.axis_index("seq_1"), lax.axis_index("seq_2")
    me = y * NX + x
    parity, pair = lax.rem(z, 2), z // 2
    turned = lax.rem(z + lax.rem(lax.axis_index("clip"), 2), 2)
    partner = lax.rem(z + 1 - 2 * turned + NZ, NZ)
    ins, outs = (tq, tk, tv, tg), (oq, ok, ov)

    def z_peer(k):
        return lax.rem(z + k, NZ)

    def plane_peer(k):
        return lax.rem(y + k // NX, 2), lax.rem(x + k % NX, NX)

    def in_plane(k):
        py, px = plane_peer(k)
        return {"seq_0": py, "seq_2": px}

    def at_z(k):
        return {"seq_1": z_peer(k % NZ)}

    barrier = pltpu.get_barrier_semaphore()
    near = [at_z(k) for k in (1, -1, 2, -2)] + [in_plane(k) for k in (1, 3, 4)]
    for device in near:
        pl.semaphore_signal(barrier, 1, device_id=device, device_id_type=MESH)

    def send(src, dst, send_sem, recv_sem, device):
        pltpu.make_async_remote_copy(
            src_ref=src, dst_ref=dst, send_sem=send_sem, recv_sem=recv_sem, device_id=device, device_id_type=MESH
        ).start()

    def wait_for(ref, sem):
        pltpu.make_async_copy(ref, ref, sem).wait()

    own = [pltpu.make_async_copy(ins[a], vin.at[a], ls.at[a]) for a in range(4)]
    cross = [pltpu.make_async_copy(*pair, ls.at[4 + i]) for i, pair in enumerate(((cq, cqb), (cg, cgb), (xk, xkb), (xv, xvb)))]
    for copy in own + cross:
        copy.start()
    for copy in own:
        copy.wait()

    def spread(c, distances):
        lanes = pl.ds(*IN_CHUNKS[c])
        for a in range(4):
            for k in distances:
                peer = z_peer(k % NZ)
                send(vin.at[a, peer, :, lanes], zbuf.at[a, z, :, lanes], zs.at[c, a], zr.at[c, a], {"seq_1": peer})

    def pass_on(i, devices):
        for device in devices:
            pl.semaphore_signal(known.at[i], 1, device_id=device, device_id_type=MESH)

    pl.semaphore_wait(barrier, len(near))
    pass_on(0, (at_z(2), at_z(-2)))
    spread(0, (2, -2, 1, -1))
    pl.semaphore_wait(known.at[0], 2)
    pass_on(1, (at_z(4), at_z(-4)))
    pass_on(2, [in_plane(k) for k in (1, 3, 4)])
    spread(0, (4, -4, 3, -3))
    pl.semaphore_wait(known.at[1], 2)
    spread(0, (8, 7, -7, 6, -6, 5, -5))
    spread(1, DISTANCES)
    for a in range(4):
        zbuf[a, z] = vin[a, z]
    for copy in cross:
        copy.wait()

    text_rows = lax.broadcasted_iota(jnp.int32, (TEXT, POS), 0)
    keep = text_rows < length[0]

    def put_cross(t, value):
        ocq[:, 128 * t : 128 * t + 128] = value.astype(BF)

    def put_text(kind):
        def put(t, value):
            tpart[kind, :, 128 * t : 128 * t + 128] = value

        return put

    sums = (Tiles(put_cross), Tiles(put_text(0)), Tiles(put_text(1)))
    for h in range(HEADS):
        low, high = window(h)
        grads = head_back(*(b[:, low:high] for b in (cqb, xkb, xvb, cgb)), head_mask(h), keep)
        for s, grad in zip(sums, grads, strict=True):
            s.add(h, grad)

    pl.semaphore_wait(known.at[2], 3)
    pass_on(3, (in_plane(4),))
    pl.semaphore_wait(known.at[3], 1)

    for k in range(1, NPL):
        py, px = plane_peer(k)
        rows, lanes = pl.ds(pl.multiple_of(px * TEXT_ROWS, 8), TEXT_ROWS), pl.ds(pl.multiple_of(py * 512, 128), HALF)
        send(tpart.at[:, rows, lanes], rs1.at[me], ts.at[0], tr.at[0], in_plane(k))
    own_rows, own_lanes = pl.ds(pl.multiple_of(x * TEXT_ROWS, 8), TEXT_ROWS), pl.ds(pl.multiple_of(y * 512, 128), HALF)
    rs1[me] = tpart[:, own_rows, own_lanes]

    def hand_on(c):
        low, size = IN_CHUNKS[c]
        lanes = pl.ds(low, size)
        for a in range(4):
            wait_for(zbuf.at[a, pl.ds(0, NZ - 1), :, lanes], zr.at[c, a])
            for t in range(low, low + size, 128):
                for f in range(NZ):
                    tall[t // 128, pl.ds(f, NPL, stride=NZ), :] = zbuf[a, f, :, t : t + 128].astype(F32)
                for j in range(NPL):
                    pout[a, j, :, t : t + 128] = tall[t // 128, NZ * j : NZ * j + NZ, :].astype(BF)
            for k in range(1, NPL):
                py, px = plane_peer(k)
                send(pout.at[a, py * NX + px, :, lanes], pbuf.at[a, me, :, lanes], ps.at[c, a], pr.at[c, a], in_plane(k))
            pbuf[a, me, :, low : low + size] = pout[a, me, :, low : low + size]

    def put_temporal(a):
        def put(t, value):
            gbuf[a, :, :, 128 * t : 128 * t + 128] = value.astype(BF).reshape(NPL, NZ, 128)

        return put

    temporal = tuple(Tiles(put_temporal(a)) for a in range(3))

    def attend(c):
        low, size = IN_CHUNKS[c]
        for a in range(4):
            wait_for(pbuf.at[a, pl.ds(0, NPL - 1), :, pl.ds(low, size)], pr.at[c, a])
        for h in range(*HEAD_CHUNKS[c]):
            lo, hi = window(h)
            q, k, v, g = (pbuf[a, :, :, lo:hi].reshape(POS, hi - lo) for a in range(4))
            for s, grad in zip(temporal, head_back(q, k, v, g, head_mask(h), None), strict=True):
                s.add(h, grad)

    def give_back(c):
        low, size = OUT_CHUNKS[c]
        lanes = pl.ds(low, size)
        for a in range(3):
            for k in range(1, NPL):
                py, px = plane_peer(k)
                send(gbuf.at[a, py * NX + px, :, lanes], qbuf.at[a, me, :, lanes], qs.at[c, a], qr.at[c, a], in_plane(k))
            qbuf[a, me, :, low : low + size] = gbuf[a, me, :, low : low + size]

    def deliver(c):
        low, size = OUT_CHUNKS[c]
        lanes = pl.ds(low, size)

        def to(peer, a):
            send(zout.at[a, peer, :, lanes], outs[a].at[z, :, lanes], ws.at[c, a], wr.at[c, a], {"seq_1": peer})

        for a in range(3):
            wait_for(qbuf.at[a, pl.ds(0, NPL - 1), :, lanes], qr.at[c, a])
            for t in range(low, low + size, 128):
                for j in range(NPL):
                    tall[t // 128, pl.ds(j, NZ, stride=NPL), :] = qbuf[a, j, :, t : t + 128].astype(F32)
                for f in range(NZ):
                    zout[a, f, :, t : t + 128] = tall[t // 128, NPL * f : NPL * f + NPL, :].astype(BF)
            pltpu.make_async_copy(zout.at[a, z, :, lanes], outs[a].at[z, :, lanes], os.at[c, a]).start()
            if c == 0:
                for k in DISTANCES:
                    to(z_peer(k), a)
        if c == 1:
            for i in range(NZ - 1):
                for a in range(3):
                    to(i + jnp.where(i >= z, 1, 0), a)

    hand_on(0)

    wait_for(rs1.at[pl.ds(0, NPL - 1)], tr.at[0])
    keys, values = (sum((rs1[j, kind] for j in range(1, NPL)), rs1[0, kind]) for kind in range(2))
    rsmine[...] = jnp.where(parity == 0, keys, values)
    rsout[...] = jnp.where(parity == 0, values, keys).astype(BF)
    send(rsout, rsin, ts.at[1], tr.at[1], {"seq_1": partner})

    attend(0)
    give_back(0)
    deliver(0)
    hand_on(1)

    wait_for(rsin, tr.at[1])
    rsmine[...] = rsmine[...] + rsin[...].astype(F32)
    for i in range(NP):
        first, second = (rsmine[:, s : s + HEAD_DIM] for s in (HEAD_DIM * i, HEAD_DIM * i + 64))
        rs2out[i] = packed(jnp.where(y == 0, first, second)).astype(BF)
    for k in PAIR_DISTANCES:
        peer = lax.rem(pair + k, NP)
        send(rs2out.at[peer], rs2.at[pair], ts.at[2], tr.at[2], {"seq_1": 2 * peer + parity})
    rs2[pair] = rs2out[pair]

    attend(1)
    give_back(1)
    deliver(1)

    wait_for(rs2.at[pl.ds(0, NP - 1)], tr.at[2])
    total = unpacked(sum((rs2[f].astype(F32) for f in range(1, NP)), rs2[0].astype(F32)))
    columns = HEAD_DIM // NX
    for j in range(NX):
        rs3out[j] = jnp.pad(total[:, columns * j : columns * j + columns], ((0, 0), (0, 128 - columns)))
    for k in range(1, NX):
        _, px = plane_peer(k)
        send(rs3out.at[px], rs3.at[x], ts.at[3], tr.at[3], in_plane(k))
    rs3[x] = rs3out[x]

    wait_for(rs3.at[pl.ds(0, NX - 1)], tr.at[3])
    otext[...] = jnp.transpose(rs3[...].reshape(TEXT, 128))[:columns, :]

    for c in range(2):
        lanes_in, lanes_out = pl.ds(*IN_CHUNKS[c]), pl.ds(*OUT_CHUNKS[c])
        for a in range(4):
            wait_for(zbuf.at[a, pl.ds(0, NZ - 1), :, lanes_in], zs.at[c, a])
            wait_for(pout.at[a, pl.ds(0, NPL - 1), :, lanes_in], ps.at[c, a])
        for a in range(3):
            wait_for(gbuf.at[a, pl.ds(0, NPL - 1), :, lanes_out], qs.at[c, a])
            wait_for(zout.at[a, pl.ds(0, NZ - 1), :, lanes_out], ws.at[c, a])
            wait_for(outs[a].at[pl.ds(0, NZ - 1), :, lanes_out], wr.at[c, a])
            wait_for(outs[a].at[0, :, lanes_out], os.at[c, a])
    wait_for(rs1.at[pl.ds(0, NPL - 1)], ts.at[0])
    wait_for(rsin, ts.at[1])
    wait_for(rs2.at[pl.ds(0, NP - 1)], ts.at[2])
    wait_for(rs3.at[pl.ds(0, NX - 1)], ts.at[3])


def move(count, *refs):
    copies = [pltpu.make_async_copy(refs[i], refs[count + i], refs[2 * count].at[i]) for i in range(count)]
    for copy in copies:
        copy.start()
    for copy in copies:
        copy.wait()


def local(tq, tk, tv, tg, cq, cg, xk, xv, length):
    arrays = [a.reshape(NZ, POS // NZ, WIDTH) for a in (tq, tk, tv, tg)]
    arrays += [cq.reshape(POS, WIDTH), cg.reshape(POS, WIDTH), xk, xv]
    vmem, dma = pltpu.VMEM, pltpu.SemaphoreType.DMA
    anywhere = pl.BlockSpec(memory_space=pl.ANY)
    block = jax.ShapeDtypeStruct((NZ, POS // NZ, WIDTH), BF)
    shapes = (
        block,
        block,
        block,
        jax.ShapeDtypeStruct((POS, WIDTH), BF),
        jax.ShapeDtypeStruct((HEAD_DIM // NX, TEXT), F32),
    )
    grads = pl.pallas_call(
        kernel,
        name="attend_back",
        out_shape=shapes,
        in_specs=[pl.BlockSpec(memory_space=pltpu.HBM)] * 8 + [pl.BlockSpec(memory_space=pltpu.SMEM)],
        out_specs=[anywhere] * 3 + [pl.BlockSpec(memory_space=vmem)] * 2,
        scratch_shapes=[
            vmem((4, NZ, 8, WIDTH), BF),
            vmem((4, NPL, NZ, WIDTH), BF),
            vmem((4, NPL, NZ, WIDTH), BF),
            vmem((3, NPL, NZ, WIDTH), BF),
            vmem((3, NPL, NZ, WIDTH), BF),
            vmem((3, NZ, 8, WIDTH), BF),
            vmem((WIDTH // 128, POS, 128), F32),
            vmem((2, TEXT, WIDTH), F32),
            vmem((NPL, 2, TEXT_ROWS, HALF), F32),
            vmem((TEXT_ROWS, HALF), BF),
            vmem((TEXT_ROWS, HALF), F32),
            vmem((TEXT_ROWS, HALF), BF),
            vmem((NP, 24, 128), BF),
            vmem((NP, 24, 128), BF),
            vmem((NX, TEXT_ROWS, 128), F32),
            vmem((NX, TEXT_ROWS, 128), F32),
            vmem((POS, WIDTH), BF),
            vmem((POS, WIDTH), BF),
            vmem((TEXT, WIDTH), BF),
            vmem((TEXT, WIDTH), BF),
            vmem((4, NZ, 8, WIDTH), BF),
            dma((2, 4)),
            dma((2, 4)),
            dma((2, 4)),
            dma((2, 4)),
            dma((2, 3)),
            dma((2, 3)),
            dma((2, 3)),
            dma((2, 3)),
            dma((4,)),
            dma((4,)),
            dma((8,)),
            dma((2, 3)),
            pltpu.SemaphoreType.REGULAR((4,)),
        ],
        compiler_params=pltpu.CompilerParams(
            collective_id=0, has_side_effects=True, vmem_limit_bytes=32 * 2**20
        ),
    )(*(pltpu.with_memory_space_constraint(a, pltpu.HBM) for a in arrays), length)
    count = len(shapes)
    oq, ok, ov, ocq, otext = pl.pallas_call(
        lambda *refs: move(count, *refs),
        name="move",
        out_shape=shapes,
        in_specs=[anywhere] * count,
        out_specs=[anywhere] * count,
        scratch_shapes=[dma((count,))],
        compiler_params=pltpu.CompilerParams(vmem_limit_bytes=2**20),
    )(*grads)
    whole = (1, POS, WIDTH)
    return oq.reshape(whole), ok.reshape(whole), ov.reshape(whole), ocq.reshape(whole), otext.T


def solution(mesh):
    torus = Mesh(mesh.devices.reshape(mesh.shape["clip"], 2, NZ, NX), CLIP_SEQ)
    tokens = P(CLIP_SEQ, None, None)
    return jax.shard_map(
        local,
        mesh=torus,
        in_specs=(tokens,) * 6 + (P("clip", None), P("clip", None), P("clip")),
        out_specs=(tokens,) * 4 + (P("clip", SEQ),),
        check_vma=False,
    )
```

```python
import math

import jax
import jax.numpy as jnp
from jax import lax
from jax.experimental import pallas as pl
from jax.experimental.pallas import tpu as pltpu
from jax.sharding import Mesh
from jax.sharding import PartitionSpec as P

HEADS = 16
HEAD_DIM = 72
WIDTH = HEADS * HEAD_DIM
POS = 128
TEXT = 160
NZ = 16
NP = NZ // 2
NX = 4
NPL = 8
SCALE = 1.0 / math.sqrt(HEAD_DIM)
CLIP_SEQ = ("clip", "seq_0", "seq_1", "seq_2")
SEQ = ("seq_0", "seq_1", "seq_2")
MESH = pl.DeviceIdType.MESH
BF = jnp.bfloat16
F32 = jnp.float32

IN_CHUNKS = ((0, 640), (640, 512))
HEAD_CHUNKS = ((0, 8), (8, 16))
OUT_CHUNKS = ((0, 512), (512, 640))
DISTANCES = (8, 7, 9, 6, 10, 5, 11, 4, 12, 3, 13, 2, 14, 1, 15)
EARLY = 7
PAIR_DISTANCES = (4, 3, 5, 2, 6, 1, 7)
TEXT_ROWS = TEXT // NX
HALF = 640


def window(head):
    low = HEAD_DIM * head // 128 * 128
    return low, -(-HEAD_DIM * (head + 1) // 128) * 128


def head_mask(head):
    low, high = window(head)
    lane = lax.broadcasted_iota(jnp.int32, (1, high - low), 1) + low
    inside = (lane >= HEAD_DIM * head) & (lane < HEAD_DIM * (head + 1))
    return jnp.where(inside, 1.0, 0.0).astype(BF)


def across(a, b):
    return lax.dot_general(a, b, (((1,), (1,)), ((), ())), preferred_element_type=F32)


def down(a, b):
    return lax.dot_general(a, b, (((0,), (0,)), ((), ())), preferred_element_type=F32)


def head_back(q, k, v, g, mask, keep):
    kz, vz, qz, gz = k * mask, v * mask, q * mask, g * mask
    scores = across(kz, q) * SCALE
    if keep is not None:
        scores = jnp.where(keep, scores, -1e30)
    expo = jnp.exp(scores - jnp.max(scores, axis=0, keepdims=True))
    weights = expo * (1.0 / jnp.sum(expo, axis=0, keepdims=True))
    rounded = weights.astype(BF)
    products = across(vz, g)
    delta = jnp.sum(rounded.astype(F32) * products, axis=0, keepdims=True)
    slopes = (weights * (products - delta) * SCALE).astype(BF)
    grad_v = jnp.dot(rounded, gz, preferred_element_type=F32)
    grad_k = jnp.dot(slopes, qz, preferred_element_type=F32)
    grad_q = down(slopes, kz)
    return grad_q, grad_k, grad_v


def packed(block):
    rows = [block[8 * r : 8 * r + 8] for r in range(5)]
    last = [rows[4][:, :64], *(row[:, 64:] for row in rows), jnp.zeros((8, 24), F32)]
    parts = ([rows[0][:, :64], rows[1][:, :64]], [rows[2][:, :64], rows[3][:, :64]], last)
    return jnp.concatenate([jnp.concatenate(part, axis=1) for part in parts], axis=0)


def unpacked(block):
    rows = [block[8 * (r // 2) : 8 * (r // 2) + 8, 64 * (r % 2) : 64 * (r % 2) + 64] for r in range(5)]
    rest = [block[16:24, 64 + 8 * r : 72 + 8 * r] for r in range(5)]
    return jnp.concatenate([jnp.concatenate(pair, axis=1) for pair in zip(rows, rest, strict=True)], axis=0)


class Tiles:
    def __init__(self, store):
        self.open, self.store = {}, store

    def add(self, head, value):
        low, high = window(head)
        for t in range(low // 128, high // 128):
            part = value[:, 128 * t - low : 128 * t - low + 128]
            self.open[t] = part if t not in self.open else self.open[t] + part
            if HEAD_DIM * (head + 1) >= 128 * (t + 1):
                self.store(t, self.open.pop(t))


def kernel(
    tq, tk, tv, tg, cq, cg, xk, xv, length,
    oq, ok, ov, ocq, otext,
    zbuf, pout, pbuf, gbuf, qbuf, zout, tall, tpart, rs1, rsout, rsmine, rsin, rs2out, rs2, rs3out, rs3, cqb, cgb, xkb, xvb, vin,
    zs, zr, ps, pr, qs, qr, ws, wr, ts, tr, ls, os, known,
):
    y, z, x = lax.axis_index("seq_0"), lax.axis_index("seq_1"), lax.axis_index("seq_2")
    me = y * NX + x
    parity, pair = lax.rem(z, 2), z // 2
    turned = lax.rem(z + lax.rem(lax.axis_index("clip"), 2), 2)
    partner = lax.rem(z + 1 - 2 * turned + NZ, NZ)
    ins, outs = (tq, tk, tv, tg), (oq, ok, ov)

    def z_peer(k):
        return lax.rem(z + k, NZ)

    def plane_peer(k):
        return lax.rem(y + k // NX, 2), lax.rem(x + k % NX, NX)

    def in_plane(k):
        py, px = plane_peer(k)
        return {"seq_0": py, "seq_2": px}

    def at_z(k):
        return {"seq_1": z_peer(k % NZ)}

    barrier = pltpu.get_barrier_semaphore()
    near = [at_z(k) for k in (1, -1, 2, -2)] + [in_plane(k) for k in (1, 3, 4)]
    for device in near:
        pl.semaphore_signal(barrier, 1, device_id=device, device_id_type=MESH)

    def send(src, dst, send_sem, recv_sem, device):
        pltpu.make_async_remote_copy(
            src_ref=src, dst_ref=dst, send_sem=send_sem, recv_sem=recv_sem, device_id=device, device_id_type=MESH
        ).start()

    def wait_for(ref, sem):
        pltpu.make_async_copy(ref, ref, sem).wait()

    own = [pltpu.make_async_copy(ins[a], vin.at[a], ls.at[a]) for a in range(4)]
    cross = [pltpu.make_async_copy(*pair, ls.at[4 + i]) for i, pair in enumerate(((cq, cqb), (cg, cgb), (xk, xkb), (xv, xvb)))]
    for copy in own + cross:
        copy.start()
    for copy in own:
        copy.wait()

    def spread(c, distances):
        lanes = pl.ds(*IN_CHUNKS[c])
        for a in range(4):
            for k in distances:
                peer = z_peer(k % NZ)
                send(vin.at[a, peer, :, lanes], zbuf.at[a, z, :, lanes], zs.at[c, a], zr.at[c, a], {"seq_1": peer})

    def pass_on(i, devices):
        for device in devices:
            pl.semaphore_signal(known.at[i], 1, device_id=device, device_id_type=MESH)

    pl.semaphore_wait(barrier, len(near))
    pass_on(0, (at_z(2), at_z(-2)))
    spread(0, (2, -2, 1, -1))
    pl.semaphore_wait(known.at[0], 2)
    pass_on(1, (at_z(4), at_z(-4)))
    pass_on(2, [in_plane(k) for k in (1, 3, 4)])
    spread(0, (4, -4, 3, -3))
    pl.semaphore_wait(known.at[1], 2)
    spread(0, (8, 7, -7, 6, -6, 5, -5))
    spread(1, DISTANCES)
    for a in range(4):
        zbuf[a, z] = vin[a, z]
    for copy in cross:
        copy.wait()

    text_rows = lax.broadcasted_iota(jnp.int32, (TEXT, POS), 0)
    keep = text_rows < length[0]

    def put_cross(t, value):
        ocq[:, 128 * t : 128 * t + 128] = value.astype(BF)

    def put_text(kind):
        def put(t, value):
            tpart[kind, :, 128 * t : 128 * t + 128] = value

        return put

    sums = (Tiles(put_cross), Tiles(put_text(0)), Tiles(put_text(1)))
    for h in range(HEADS):
        low, high = window(h)
        grads = head_back(*(b[:, low:high] for b in (cqb, xkb, xvb, cgb)), head_mask(h), keep)
        for s, grad in zip(sums, grads, strict=True):
            s.add(h, grad)

    pl.semaphore_wait(known.at[2], 3)
    pass_on(3, (in_plane(4),))
    pl.semaphore_wait(known.at[3], 1)

    for k in range(1, NPL):
        py, px = plane_peer(k)
        rows, lanes = pl.ds(pl.multiple_of(px * TEXT_ROWS, 8), TEXT_ROWS), pl.ds(pl.multiple_of(py * 512, 128), HALF)
        send(tpart.at[:, rows, lanes], rs1.at[me], ts.at[0], tr.at[0], in_plane(k))
    own_rows, own_lanes = pl.ds(pl.multiple_of(x * TEXT_ROWS, 8), TEXT_ROWS), pl.ds(pl.multiple_of(y * 512, 128), HALF)
    rs1[me] = tpart[:, own_rows, own_lanes]

    def hand_on(c):
        low, size = IN_CHUNKS[c]
        lanes = pl.ds(low, size)
        for a in range(4):
            wait_for(zbuf.at[a, pl.ds(0, NZ - 1), :, lanes], zr.at[c, a])
            for t in range(low, low + size, 128):
                for f in range(NZ):
                    tall[t // 128, pl.ds(f, NPL, stride=NZ), :] = zbuf[a, f, :, t : t + 128].astype(F32)
                for j in range(NPL):
                    pout[a, j, :, t : t + 128] = tall[t // 128, NZ * j : NZ * j + NZ, :].astype(BF)
            for k in range(1, NPL):
                py, px = plane_peer(k)
                send(pout.at[a, py * NX + px, :, lanes], pbuf.at[a, me, :, lanes], ps.at[c, a], pr.at[c, a], in_plane(k))
            pbuf[a, me, :, low : low + size] = pout[a, me, :, low : low + size]

    def put_temporal(a):
        def put(t, value):
            gbuf[a, :, :, 128 * t : 128 * t + 128] = value.astype(BF).reshape(NPL, NZ, 128)

        return put

    temporal = tuple(Tiles(put_temporal(a)) for a in range(3))

    def attend(c):
        low, size = IN_CHUNKS[c]
        for a in range(4):
            wait_for(pbuf.at[a, pl.ds(0, NPL - 1), :, pl.ds(low, size)], pr.at[c, a])
        for h in range(*HEAD_CHUNKS[c]):
            lo, hi = window(h)
            q, k, v, g = (pbuf[a, :, :, lo:hi].reshape(POS, hi - lo) for a in range(4))
            for s, grad in zip(temporal, head_back(q, k, v, g, head_mask(h), None), strict=True):
                s.add(h, grad)

    def give_back(c):
        low, size = OUT_CHUNKS[c]
        lanes = pl.ds(low, size)
        for a in range(3):
            for k in range(1, NPL):
                py, px = plane_peer(k)
                send(gbuf.at[a, py * NX + px, :, lanes], qbuf.at[a, me, :, lanes], qs.at[c, a], qr.at[c, a], in_plane(k))
            qbuf[a, me, :, low : low + size] = gbuf[a, me, :, low : low + size]

    def deliver(c):
        low, size = OUT_CHUNKS[c]
        lanes = pl.ds(low, size)

        def to(peer, a):
            send(zout.at[a, peer, :, lanes], outs[a].at[z, :, lanes], ws.at[c, a], wr.at[c, a], {"seq_1": peer})

        for a in range(3):
            wait_for(qbuf.at[a, pl.ds(0, NPL - 1), :, lanes], qr.at[c, a])
            for t in range(low, low + size, 128):
                for j in range(NPL):
                    tall[t // 128, pl.ds(j, NZ, stride=NPL), :] = qbuf[a, j, :, t : t + 128].astype(F32)
                for f in range(NZ):
                    zout[a, f, :, t : t + 128] = tall[t // 128, NPL * f : NPL * f + NPL, :].astype(BF)
            pltpu.make_async_copy(zout.at[a, z, :, lanes], outs[a].at[z, :, lanes], os.at[c, a]).start()
            if c == 0:
                for k in DISTANCES:
                    to(z_peer(k), a)
            elif a == 0:
                for i in range(EARLY):
                    to(i + jnp.where(i >= z, 1, 0), a)
        if c == 1:
            for i in range(NZ - 1):
                for a in range(1 if i < EARLY else 0, 3):
                    to(i + jnp.where(i >= z, 1, 0), a)

    hand_on(0)

    wait_for(rs1.at[pl.ds(0, NPL - 1)], tr.at[0])
    keys, values = (sum((rs1[j, kind] for j in range(1, NPL)), rs1[0, kind]) for kind in range(2))
    rsmine[...] = jnp.where(parity == 0, keys, values)
    rsout[...] = jnp.where(parity == 0, values, keys).astype(BF)
    send(rsout, rsin, ts.at[1], tr.at[1], {"seq_1": partner})

    attend(0)
    give_back(0)
    deliver(0)
    hand_on(1)

    wait_for(rsin, tr.at[1])
    rsmine[...] = rsmine[...] + rsin[...].astype(F32)
    for i in range(NP):
        first, second = (rsmine[:, s : s + HEAD_DIM] for s in (HEAD_DIM * i, HEAD_DIM * i + 64))
        rs2out[i] = packed(jnp.where(y == 0, first, second)).astype(BF)
    for k in PAIR_DISTANCES:
        peer = lax.rem(pair + k, NP)
        send(rs2out.at[peer], rs2.at[pair], ts.at[2], tr.at[2], {"seq_1": 2 * peer + parity})
    rs2[pair] = rs2out[pair]

    attend(1)
    give_back(1)
    deliver(1)

    wait_for(rs2.at[pl.ds(0, NP - 1)], tr.at[2])
    total = unpacked(sum((rs2[f].astype(F32) for f in range(1, NP)), rs2[0].astype(F32)))
    columns = HEAD_DIM // NX
    for j in range(NX):
        rs3out[j] = jnp.pad(total[:, columns * j : columns * j + columns], ((0, 0), (0, 128 - columns)))
    for k in range(1, NX):
        _, px = plane_peer(k)
        send(rs3out.at[px], rs3.at[x], ts.at[3], tr.at[3], in_plane(k))
    rs3[x] = rs3out[x]

    wait_for(rs3.at[pl.ds(0, NX - 1)], tr.at[3])
    otext[...] = jnp.transpose(rs3[...].reshape(TEXT, 128))[:columns, :]

    for c in range(2):
        lanes_in, lanes_out = pl.ds(*IN_CHUNKS[c]), pl.ds(*OUT_CHUNKS[c])
        for a in range(4):
            wait_for(zbuf.at[a, pl.ds(0, NZ - 1), :, lanes_in], zs.at[c, a])
            wait_for(pout.at[a, pl.ds(0, NPL - 1), :, lanes_in], ps.at[c, a])
        for a in range(3):
            wait_for(gbuf.at[a, pl.ds(0, NPL - 1), :, lanes_out], qs.at[c, a])
            wait_for(zout.at[a, pl.ds(0, NZ - 1), :, lanes_out], ws.at[c, a])
            wait_for(outs[a].at[pl.ds(0, NZ - 1), :, lanes_out], wr.at[c, a])
            wait_for(outs[a].at[0, :, lanes_out], os.at[c, a])
    wait_for(rs1.at[pl.ds(0, NPL - 1)], ts.at[0])
    wait_for(rsin, ts.at[1])
    wait_for(rs2.at[pl.ds(0, NP - 1)], ts.at[2])
    wait_for(rs3.at[pl.ds(0, NX - 1)], ts.at[3])


def move(count, *refs):
    copies = [pltpu.make_async_copy(refs[i], refs[count + i], refs[2 * count].at[i]) for i in range(count)]
    for copy in copies:
        copy.start()
    for copy in copies:
        copy.wait()


def local(tq, tk, tv, tg, cq, cg, xk, xv, length):
    arrays = [a.reshape(NZ, POS // NZ, WIDTH) for a in (tq, tk, tv, tg)]
    arrays += [cq.reshape(POS, WIDTH), cg.reshape(POS, WIDTH), xk, xv]
    vmem, dma = pltpu.VMEM, pltpu.SemaphoreType.DMA
    anywhere = pl.BlockSpec(memory_space=pl.ANY)
    block = jax.ShapeDtypeStruct((NZ, POS // NZ, WIDTH), BF)
    shapes = (
        block,
        block,
        block,
        jax.ShapeDtypeStruct((POS, WIDTH), BF),
        jax.ShapeDtypeStruct((HEAD_DIM // NX, TEXT), F32),
    )
    grads = pl.pallas_call(
        kernel,
        name="attend_back",
        out_shape=shapes,
        in_specs=[pl.BlockSpec(memory_space=pltpu.HBM)] * 8 + [pl.BlockSpec(memory_space=pltpu.SMEM)],
        out_specs=[anywhere] * 3 + [pl.BlockSpec(memory_space=vmem)] * 2,
        scratch_shapes=[
            vmem((4, NZ, 8, WIDTH), BF),
            vmem((4, NPL, NZ, WIDTH), BF),
            vmem((4, NPL, NZ, WIDTH), BF),
            vmem((3, NPL, NZ, WIDTH), BF),
            vmem((3, NPL, NZ, WIDTH), BF),
            vmem((3, NZ, 8, WIDTH), BF),
            vmem((WIDTH // 128, POS, 128), F32),
            vmem((2, TEXT, WIDTH), F32),
            vmem((NPL, 2, TEXT_ROWS, HALF), F32),
            vmem((TEXT_ROWS, HALF), BF),
            vmem((TEXT_ROWS, HALF), F32),
            vmem((TEXT_ROWS, HALF), BF),
            vmem((NP, 24, 128), BF),
            vmem((NP, 24, 128), BF),
            vmem((NX, TEXT_ROWS, 128), F32),
            vmem((NX, TEXT_ROWS, 128), F32),
            vmem((POS, WIDTH), BF),
            vmem((POS, WIDTH), BF),
            vmem((TEXT, WIDTH), BF),
            vmem((TEXT, WIDTH), BF),
            vmem((4, NZ, 8, WIDTH), BF),
            dma((2, 4)),
            dma((2, 4)),
            dma((2, 4)),
            dma((2, 4)),
            dma((2, 3)),
            dma((2, 3)),
            dma((2, 3)),
            dma((2, 3)),
            dma((4,)),
            dma((4,)),
            dma((8,)),
            dma((2, 3)),
            pltpu.SemaphoreType.REGULAR((4,)),
        ],
        compiler_params=pltpu.CompilerParams(
            collective_id=0, has_side_effects=True, vmem_limit_bytes=32 * 2**20
        ),
    )(*(pltpu.with_memory_space_constraint(a, pltpu.HBM) for a in arrays), length)
    count = len(shapes)
    oq, ok, ov, ocq, otext = pl.pallas_call(
        lambda *refs: move(count, *refs),
        name="move",
        out_shape=shapes,
        in_specs=[anywhere] * count,
        out_specs=[anywhere] * count,
        scratch_shapes=[dma((count,))],
        compiler_params=pltpu.CompilerParams(vmem_limit_bytes=2**20),
    )(*grads)
    whole = (1, POS, WIDTH)
    return oq.reshape(whole), ok.reshape(whole), ov.reshape(whole), ocq.reshape(whole), otext.T


def solution(mesh):
    torus = Mesh(mesh.devices.reshape(mesh.shape["clip"], 2, NZ, NX), CLIP_SEQ)
    tokens = P(CLIP_SEQ, None, None)
    return jax.shard_map(
        local,
        mesh=torus,
        in_specs=(tokens,) * 6 + (P("clip", None), P("clip", None), P("clip")),
        out_specs=(tokens,) * 4 + (P("clip", SEQ),),
        check_vma=False,
    )
```
